32 devices in a mesh: data: 4 (over y, z), fsdp: 8 (over x, core).
Axes of the slice: x: 4, y: 2, z: 2, core: 2. Of those that a mesh axis runs over, the one named last changes fastest.
The devices are a block of a 4x4x8 slice.
Arguments:
- hidden: bfloat16 [16384, 768], P('data'), parts along dimension 0
- targets: int32 [16384], P('data'), parts along dimension 0
- w_out: bfloat16 [50304, 768], P('fsdp')
Outputs:
- output 1: float32 [4], P('data'), parts along dimension 0
- output 2: float32 [16384, 768], P(('data', 'fsdp')), parts along dimension 0
- output 3: float32 [201216, 768], P(('data', 'fsdp')), parts along dimension 0
There are 4 independent parts. The reference program is written for one: setup_inputs(seed, part) draws one part's arguments, and reference() takes and returns one part's arrays. A program takes and returns all parts, laid end to end along the dimension named above; an argument that names none is the same for every part.
All inputs are finite; a program needn't handle non-finite values.
Results may differ from the reference program's by a relative error of at most 0.001.
Values are sent between devices in bfloat16 or wider.
A program may use at most 768 MiB of HBM per device.

```python
import math
import jax
import jax.numpy as jnp
from jax import lax

GROUP_SIZE = 8
TOKENS_DEV = 512
VOCAB_SIZE = 50304
MODEL_DIM = 768

TOKENS = TOKENS_DEV * GROUP_SIZE
VOCAB_DEV = VOCAB_SIZE // GROUP_SIZE


def setup_inputs(seed: int = 0, part: int = 0) -> dict:
    base_key = jax.random.key(seed)
    shared_key, part_base = jax.random.split(base_key)
    part_key = jax.random.fold_in(part_base, part)
    noise_key, offset_key, perm_key = jax.random.split(part_key, 3)
    w_out = (jax.random.normal(shared_key, (VOCAB_SIZE, MODEL_DIM), jnp.float32) * MODEL_DIM ** -0.5).astype(jnp.bfloat16)
    positions = jnp.arange(TOKENS)
    offsets = jax.random.randint(offset_key, (TOKENS,), 0, VOCAB_DEV)
    offsets = jnp.where(positions == 0, 0, offsets)
    offsets = jnp.where(positions == GROUP_SIZE - 1, VOCAB_DEV - 1, offsets)
    targets = jax.random.permutation(perm_key, (positions % GROUP_SIZE) * VOCAB_DEV + offsets).astype(jnp.int32)
    boost = math.log(VOCAB_SIZE)
    hidden = jax.random.normal(noise_key, (TOKENS, MODEL_DIM), jnp.float32) + boost * w_out.astype(jnp.float32)[targets]
    return {"hidden": hidden.astype(jnp.bfloat16), "targets": targets, "w_out": w_out}


def reference(hidden, targets, w_out):
    hid_blocks = hidden.reshape(GROUP_SIZE, TOKENS_DEV, MODEL_DIM)
    tgt_blocks = targets.reshape(GROUP_SIZE, TOKENS_DEV)
    vocab_ids = jnp.arange(VOCAB_SIZE)[None, :]

    def scan_step(grad_w, blocks):
        hid_blk, tgt_blk = blocks
        logits = jnp.dot(hid_blk, w_out.T, preferred_element_type=jnp.float32)
        row_max = jnp.max(logits, axis=1, keepdims=True)
        log_norm = row_max + jnp.log(jnp.sum(jnp.exp(logits - row_max), axis=1, keepdims=True))
        tgt_hit = vocab_ids == tgt_blk[:, None]
        tgt_logit = jnp.sum(jnp.where(tgt_hit, logits, 0.0), axis=1, keepdims=True)
        probs = jnp.exp(logits - log_norm)
        grad_logits = ((probs - tgt_hit.astype(jnp.float32)) / TOKENS).astype(jnp.bfloat16)
        grad_hid = jnp.dot(grad_logits, w_out, preferred_element_type=jnp.float32)
        grad_w = grad_w + jnp.dot(grad_logits.T, hid_blk, preferred_element_type=jnp.float32)
        return grad_w, (jnp.sum(log_norm - tgt_logit), grad_hid)

    grad_w, (loss_terms, grad_hid) = lax.scan(scan_step, jnp.zeros((VOCAB_SIZE, MODEL_DIM), jnp.float32), (hid_blocks, tgt_blocks))
    loss_val = (jnp.sum(loss_terms) / TOKENS).reshape(1)
    return loss_val, grad_hid.reshape(TOKENS, MODEL_DIM), grad_w
```

```python
import functools

import jax
import jax.numpy as jnp
from jax import lax
from jax.experimental import pallas as pl
from jax.experimental.pallas import tpu as pltpu
from jax.sharding import PartitionSpec as P

MESH = pl.DeviceIdType.MESH
AXIS = "fsdp"
TILE = 1024
VMEM_LIMIT = 67043328


def tiles_of(vocab, tile):
    count = vocab // tile
    return [(j * tile, tile if j < count - 1 else vocab - j * tile) for j in range(count)]


def stats_kernel(n, tile, h_ref, w_ref, tgt_ref, z_hbm, lse_ref, loss_ref, zbuf, stat, recv, zsem, send_sem, recv_sem):
    c = pl.program_id(0)
    p = lax.rem(c, 2)
    me = lax.axis_index(AXIS)
    vocab, t = w_ref.shape[0], h_ref.shape[0]

    @pl.when(c == 0)
    def _():
        barrier = pltpu.get_barrier_semaphore()
        for r in range(1, n):
            pl.semaphore_signal(barrier, inc=1, device_id={AXIS: lax.rem(me + r, n)}, device_id_type=MESH)
        pl.semaphore_wait(barrier, n - 1)
        stat[...] = jnp.zeros_like(stat)

    def send(chunk):
        for r in range(1, n):
            pltpu.make_async_remote_copy(
                src_ref=stat.at[chunk],
                dst_ref=recv.at[chunk, r - 1],
                send_sem=send_sem,
                recv_sem=recv_sem,
                device_id={AXIS: lax.rem(me + r, n)},
                device_id_type=MESH,
            ).start()

    @pl.when(c >= 1)
    def _():
        send(c - 1)

    @pl.when(c >= 2)
    def _():
        pltpu.make_async_copy(zbuf.at[p], z_hbm.at[c - 2], zsem.at[p]).wait()

    tgt = tgt_ref[c] - me * vocab
    m = s = hit_sum = None
    for r0, rows in tiles_of(vocab, tile):
        z = lax.dot_general(
            w_ref[r0 : r0 + rows, :], h_ref[...], (((1,), (1,)), ((), ())), preferred_element_type=jnp.float32
        )
        zbuf[p, r0 : r0 + rows, :] = z
        pltpu.make_async_copy(zbuf.at[p, pl.ds(r0, rows)], z_hbm.at[c, pl.ds(r0, rows)], zsem.at[p]).start()
        tile_max = jnp.max(z, axis=0, keepdims=True)
        new_m = tile_max if m is None else jnp.maximum(m, tile_max)
        tile_sum = jnp.sum(jnp.exp(z - new_m), axis=0, keepdims=True)
        hit = lax.broadcasted_iota(jnp.int32, (rows, t), 0) == tgt - r0
        tile_hit = jnp.sum(jnp.where(hit, z, 0.0), axis=0, keepdims=True)
        if m is None:
            s, hit_sum = tile_sum, tile_hit
        else:
            s = s * jnp.exp(m - new_m) + tile_sum
            hit_sum = hit_sum + tile_hit
        m = new_m
    stat[c, 0:1, :] = m
    stat[c, 1:2, :] = s
    stat[c, 2:3, :] = hit_sum

    @pl.when(c == n - 1)
    def _():
        send(c)
        pltpu.make_async_copy(zbuf.at[1 - p], z_hbm.at[c - 1], zsem.at[1 - p]).wait()
        pltpu.make_async_copy(zbuf.at[p], z_hbm.at[c], zsem.at[p]).wait()
        pltpu.make_async_copy(recv, recv, send_sem).wait()
        pltpu.make_async_copy(recv, recv, recv_sem).wait()
        total = jnp.zeros((1, 1), jnp.float32)
        for k in range(n):
            big = stat[k, 0:1, :]
            for r in range(n - 1):
                big = jnp.maximum(big, recv[k, r, 0:1, :])
            own = stat[k, 1:2, :] * jnp.exp(stat[k, 0:1, :] - big)
            parts = [recv[k, r, 1:2, :] * jnp.exp(recv[k, r, 0:1, :] - big) for r in range(n - 1)]
            sums = stat_sum(n, me, own, parts)
            target = stat[k, 2:3, :]
            for r in range(n - 1):
                target = target + recv[k, r, 2:3, :]
            lse = big + jnp.log(sums)
            lse_ref[k] = lse
            total = total + jnp.sum(lse - target, axis=1, keepdims=True)
        loss_ref[...] = jnp.broadcast_to(total / (n * t), loss_ref.shape)


def stat_sum(n, me, own, parts):
    total = None
    for a in range(n):
        r = lax.rem(me - a + n, n)
        term = own
        for k in range(1, n):
            term = jnp.where(r == k, parts[k - 1], term)
        total = term if total is None else total + term
    return total


def run_stats(n, tile, hidden, targets, w_blk, collective_id):
    tok, d = hidden.shape
    vocab = w_blk.shape[0]
    t = tok // n
    return pl.pallas_call(
        functools.partial(stats_kernel, n, tile),
        grid=(n,),
        in_specs=[
            pl.BlockSpec((t, d), lambda c: (c, 0)),
            pl.BlockSpec((vocab, d), lambda c: (0, 0), pipeline_mode=pl.Buffered(1)),
            pl.BlockSpec((n, 1, t), lambda c: (0, 0, 0)),
        ],
        out_specs=[
            pl.BlockSpec(memory_space=pl.ANY),
            pl.BlockSpec((n, 1, t), lambda c: (0, 0, 0)),
            pl.BlockSpec((8, 128), lambda c: (0, 0)),
        ],
        out_shape=[
            jax.ShapeDtypeStruct((n, vocab, t), jnp.float32),
            jax.ShapeDtypeStruct((n, 1, t), jnp.float32),
            jax.ShapeDtypeStruct((8, 128), jnp.float32),
        ],
        scratch_shapes=[
            pltpu.VMEM((2, vocab, t), jnp.float32),
            pltpu.VMEM((n, 8, t), jnp.float32),
            pltpu.VMEM((n, n - 1, 8, t), jnp.float32),
            pltpu.SemaphoreType.DMA((2,)),
            pltpu.SemaphoreType.DMA,
            pltpu.SemaphoreType.DMA,
        ],
        compiler_params=pltpu.CompilerParams(
            dimension_semantics=("arbitrary",),
            collective_id=collective_id,
            has_side_effects=True,
            vmem_limit_bytes=VMEM_LIMIT,
        ),
        name="stats",
    )(hidden, w_blk, targets)


def grad_kernel(
    n, tile, wt_hbm, h_hbm, z_hbm, lse_ref, tgt_ref, dht_ref, dw_hbm,
    wt, hbuf, zin, dz0, dz1, dw, hacc, from_partner, from_ring,
    wsem, hsem, zsem, dwsem, p_send, p_recv, r_send, r_recv,
):
    me = lax.axis_index(AXIS)
    nx = n // 2
    x, core = lax.div(me, 2), lax.rem(me, 2)
    sgn = 1 - 2 * core
    d, t = dht_ref.shape
    vocab = dw.shape[0]
    tiles = tiles_of(vocab, tile)
    last = len(tiles) - 1
    dz = (dz0, dz1)
    partner = 2 * x + (1 - core)
    ahead = 2 * lax.rem(x + sgn + nx, nx) + core
    behind = 2 * lax.rem(x - sgn + nx, nx) + core

    def chunk_of(s):
        q, mine = lax.div(s, 2), lax.rem(s, 2)
        e = sgn * (2 * mine - 1)
        off = jnp.where(q == 0, 2, jnp.where(q == 1, e, jnp.where(q == 2, -e, 0)))
        owner_core = core * mine + (1 - core) * (1 - mine)
        return 2 * lax.rem(x + off + nx, nx) + owner_core

    def z_copy(chunk, j):
        r0, rows = tiles[j]
        return pltpu.make_async_copy(
            z_hbm.at[chunk, pl.ds(r0, rows)], zin.at[j % 3, pl.ds(0, rows)], zsem.at[j % 3]
        )

    def h_copy(chunk, slot):
        return pltpu.make_async_copy(h_hbm.at[pl.ds(chunk * t, t)], hbuf.at[slot], hsem.at[slot])

    def make_dz(chunk, j):
        r0, rows = tiles[j]
        z = zin[j % 3, 0:rows, :]
        hit = lax.broadcasted_iota(jnp.int32, (rows, t), 0) == tgt_ref[chunk] - (me * vocab + r0)
        g = (jnp.exp(z - lse_ref[chunk]) - jnp.where(hit, 1.0, 0.0)) * (1.0 / (n * t))
        dz[j % 2][0:rows, :] = g.astype(jnp.bfloat16)

    first = chunk_of(0)
    w_copy = pltpu.make_async_copy(wt_hbm, wt, wsem)
    h_copy(first, 0).start()
    for j in range(3):
        z_copy(first, j).start()
    w_copy.start()

    barrier = pltpu.get_barrier_semaphore()
    for peer in (partner, ahead, behind):
        pl.semaphore_signal(barrier, inc=1, device_id={AXIS: peer}, device_id_type=MESH)
    pl.semaphore_wait(barrier, 3)

    def partner_copy(q):
        return pltpu.make_async_remote_copy(
            src_ref=hacc.at[0], dst_ref=from_partner.at[q], send_sem=p_send.at[q], recv_sem=p_recv.at[q],
            device_id={AXIS: partner}, device_id_type=MESH,
        )

    def ring_copy(q, peer):
        return pltpu.make_async_remote_copy(
            src_ref=hacc.at[1 + lax.rem(q, 2)], dst_ref=from_ring.at[q], send_sem=r_send.at[q], recv_sem=r_recv.at[q],
            device_id={AXIS: peer}, device_id_type=MESH,
        )

    step = max(r for r in range(16, 129, 16) if vocab % r == 0)

    def zero(i, carry):
        dw[pl.ds(i * step, step), :] = jnp.zeros((step, d), jnp.float32)
        return carry

    lax.fori_loop(0, vocab // step, zero, 0)
    pad = dz1.shape[0] - tiles[last][1]
    if pad:
        dz1[tiles[last][1] :, :] = jnp.zeros((pad, t), jnp.bfloat16)
    z_copy(first, 0).wait()
    make_dz(first, 0)
    w_copy.wait()

    def stage(s, carry):
        chunk, following = chunk_of(s), chunk_of(jnp.minimum(s + 1, n - 1))
        q, mine = lax.div(s, 2), lax.rem(s, 2)
        slot = lax.rem(s, 2)
        acc = mine * (1 + lax.rem(q, 2))
        pq, pmine = lax.div(s - 1, 2), lax.rem(s + 1, 2)
        pacc = 1 + lax.rem(pq, 2)

        @pl.when(s < n - 1)
        def _():
            h_copy(following, 1 - slot).start()

        @pl.when(jnp.logical_and(mine == 0, q >= 1))
        def _():
            partner_copy(q - 1).wait_send()

        @pl.when(jnp.logical_and(mine == 1, q >= 2))
        def _():
            ring_copy(q - 2, ahead).wait_send()

        h_copy(chunk, slot).wait()
        for j, (r0, rows) in enumerate(tiles):
            nxt = j + 1
            if nxt <= last:
                z_copy(chunk, nxt).wait()
                make_dz(chunk, nxt)
            else:

                @pl.when(s < n - 1)
                def _():
                    z_copy(following, 0).wait()

                make_dz(following, 0)
            cols = rows if j < last else dz1.shape[0]
            part = jnp.dot(wt[:, r0 : r0 + cols], dz[j % 2][0:cols, :], preferred_element_type=jnp.float32)
            if j == 0:
                hacc[acc] = part
            else:
                hacc[acc] = hacc[acc] + part
            dw[r0 : r0 + rows, :] = dw[r0 : r0 + rows, :] + jnp.dot(
                dz[j % 2][0:rows, :], hbuf[slot], preferred_element_type=jnp.float32
            )

            if j + 3 <= last:
                z_copy(chunk, j + 3).start()
            else:

                @pl.when(s < n - 1)
                def _():
                    z_copy(following, j + 3 - last - 1).start()

            @pl.when(s == n - 1)
            def _():
                pltpu.make_async_copy(dw.at[pl.ds(r0, rows)], dw_hbm.at[pl.ds(r0, rows)], dwsem).start()

            if j == 0:

                @pl.when(jnp.logical_and(s >= 1, pmine == 1))
                def _():
                    partner_copy(pq).wait_recv()
                    hacc[pacc] = hacc[pacc] + from_partner[pq]

                    @pl.when(pq == 1)
                    def _():
                        ring_copy(0, ahead).wait_recv()
                        hacc[pacc] = hacc[pacc] + from_ring[0]

            if j == 1:

                @pl.when(jnp.logical_and(s >= 1, pmine == 0))
                def _():
                    partner_copy(pq).start()

                @pl.when(jnp.logical_and(s >= 1, jnp.logical_and(pmine == 1, pq < 2)))
                def _():
                    ring_copy(pq, ahead).start()

                @pl.when(jnp.logical_and(s >= 1, jnp.logical_and(pmine == 1, pq == 2)))
                def _():
                    ring_copy(2, behind).start()

        return carry

    lax.fori_loop(0, n, stage, 0)

    partner_copy(3).wait_recv()
    ring_copy(1, ahead).wait_recv()
    total = hacc[2] + from_partner[3] + from_ring[1]
    ring_copy(2, behind).wait_recv()
    dht_ref[...] = total + from_ring[2]
    partner_copy(3).wait_send()
    ring_copy(2, behind).wait_send()
    pltpu.make_async_copy(dw, dw_hbm, dwsem).wait()


def run_grads(n, tile, w_t, hidden, z, lse, targets, collective_id):
    tok, d = hidden.shape
    vocab = z.shape[1]
    t = tok // n
    rows = tiles_of(vocab, tile)[-1][1]
    last_cols = w_t.shape[1] - (vocab - rows)
    any_spec = pl.BlockSpec(memory_space=pl.ANY)
    vmem_spec = pl.BlockSpec(memory_space=pltpu.VMEM)
    return pl.pallas_call(
        functools.partial(grad_kernel, n, tile),
        in_specs=[any_spec, any_spec, any_spec, vmem_spec, vmem_spec],
        out_specs=[vmem_spec, any_spec],
        out_shape=[
            jax.ShapeDtypeStruct((d, t), jnp.float32),
            jax.ShapeDtypeStruct((vocab, d), jnp.float32),
        ],
        scratch_shapes=[
            pltpu.VMEM(w_t.shape, jnp.bfloat16),
            pltpu.VMEM((2, t, d), jnp.bfloat16),
            pltpu.VMEM((3, rows, t), jnp.float32),
            pltpu.VMEM((tile, t), jnp.bfloat16),
            pltpu.VMEM((last_cols, t), jnp.bfloat16),
            pltpu.VMEM((vocab, d), jnp.float32),
            pltpu.VMEM((3, d, t), jnp.float32),
            pltpu.VMEM((4, d, t), jnp.float32),
            pltpu.VMEM((3, d, t), jnp.float32),
            pltpu.SemaphoreType.DMA,
            pltpu.SemaphoreType.DMA((2,)),
            pltpu.SemaphoreType.DMA((3,)),
            pltpu.SemaphoreType.DMA,
            pltpu.SemaphoreType.DMA((4,)),
            pltpu.SemaphoreType.DMA((4,)),
            pltpu.SemaphoreType.DMA((3,)),
            pltpu.SemaphoreType.DMA((3,)),
        ],
        compiler_params=pltpu.CompilerParams(
            collective_id=collective_id, has_side_effects=True, vmem_limit_bytes=VMEM_LIMIT
        ),
        name="grads",
    )(w_t, hidden, z, lse, targets)


def solution(mesh, tile=TILE):
    n = mesh.shape[AXIS]

    def local_step(hidden, targets, w_blk):
        tok = hidden.shape[0]
        vocab = w_blk.shape[0]
        tgt = targets.reshape(n, 1, tok // n)
        z, lse, loss = run_stats(n, tile, hidden, tgt, w_blk, 0)
        last_start = tiles_of(vocab, tile)[-1][0]
        padded = last_start + -(-(vocab - last_start) // 256) * 256
        w_t = jnp.pad(w_blk.T, ((0, 0), (0, padded - vocab)))
        dht, dw = run_grads(n, tile, w_t, hidden, z, lse, tgt, 1)
        return loss[0, :1], dht.T, dw

    return jax.shard_map(
        local_step,
        mesh=mesh,
        in_specs=(P("data", None), P("data"), P(AXIS, None)),
        out_specs=(P("data"), P(("data", AXIS), None), P(("data", AXIS), None)),
        check_vma=False,
    )
```

```python
import functools

import jax
import jax.numpy as jnp
from jax import lax
from jax.experimental import pallas as pl
from jax.experimental.pallas import tpu as pltpu
from jax.sharding import PartitionSpec as P

MESH = pl.DeviceIdType.MESH
AXIS = "fsdp"
TILE = 1024
PIECE = 256
ROWS = 528
VMEM_LIMIT = 67043328


def blocks_of(start, count, size):
    blocks = max(count // size, 1)
    return [(start + i * size, size if i < blocks - 1 else count - i * size) for i in range(blocks)]


def stats_kernel(n, tile, h_ref, w_ref, tgt_ref, z_hbm, lse_ref, loss_ref, zbuf, stat, recv, zsem, send_sem, recv_sem):
    c = pl.program_id(0)
    p = lax.rem(c, 2)
    me = lax.axis_index(AXIS)
    vocab, t = w_ref.shape[0], h_ref.shape[0]

    @pl.when(c == 0)
    def _():
        barrier = pltpu.get_barrier_semaphore()
        for r in range(1, n):
            pl.semaphore_signal(barrier, inc=1, device_id={AXIS: lax.rem(me + r, n)}, device_id_type=MESH)
        pl.semaphore_wait(barrier, n - 1)
        stat[...] = jnp.zeros_like(stat)

    def send(chunk):
        for r in range(1, n):
            pltpu.make_async_remote_copy(
                src_ref=stat.at[chunk],
                dst_ref=recv.at[chunk, r - 1],
                send_sem=send_sem,
                recv_sem=recv_sem,
                device_id={AXIS: lax.rem(me + r, n)},
                device_id_type=MESH,
            ).start()

    @pl.when(c >= 1)
    def _():
        send(c - 1)

    @pl.when(c >= 2)
    def _():
        pltpu.make_async_copy(zbuf.at[p], z_hbm.at[c - 2], zsem.at[p]).wait()

    tgt = tgt_ref[c] - me * vocab
    maxima, totals, hits = [], [], []
    for r0, rows in blocks_of(0, vocab, PIECE):
        z = lax.dot_general(
            w_ref[r0 : r0 + rows, :], h_ref[...], (((1,), (1,)), ((), ())), preferred_element_type=jnp.float32
        )
        zbuf[p, r0 : r0 + rows, :] = z
        big = jnp.max(z, axis=0, keepdims=True)
        total = jnp.sum(jnp.exp(z - big), axis=0, keepdims=True)
        hit = lax.broadcasted_iota(jnp.int32, (rows, t), 0) == tgt - r0
        maxima.append(big)
        totals.append(total)
        hits.append(jnp.sum(jnp.where(hit, z, 0.0), axis=0, keepdims=True))
    for r0, rows in blocks_of(0, vocab, tile):
        pltpu.make_async_copy(zbuf.at[p, pl.ds(r0, rows)], z_hbm.at[c, pl.ds(r0, rows)], zsem.at[p]).start()
    m = functools.reduce(jnp.maximum, maxima)
    stat[c, 0:1, :] = m
    stat[c, 1:2, :] = sum(s * jnp.exp(big - m) for s, big in zip(totals, maxima))
    stat[c, 2:3, :] = sum(hits)

    @pl.when(c == n - 1)
    def _():
        send(c)
        pltpu.make_async_copy(zbuf.at[1 - p], z_hbm.at[c - 1], zsem.at[1 - p]).wait()
        pltpu.make_async_copy(zbuf.at[p], z_hbm.at[c], zsem.at[p]).wait()
        pltpu.make_async_copy(recv, recv, send_sem).wait()
        pltpu.make_async_copy(recv, recv, recv_sem).wait()
        total = jnp.zeros((1, 1), jnp.float32)
        for k in range(n):
            big = stat[k, 0:1, :]
            for r in range(n - 1):
                big = jnp.maximum(big, recv[k, r, 0:1, :])
            own = stat[k, 1:2, :] * jnp.exp(stat[k, 0:1, :] - big)
            parts = [recv[k, r, 1:2, :] * jnp.exp(recv[k, r, 0:1, :] - big) for r in range(n - 1)]
            sums = stat_sum(n, me, own, parts)
            target = stat[k, 2:3, :]
            for r in range(n - 1):
                target = target + recv[k, r, 2:3, :]
            lse = big + jnp.log(sums)
            lse_ref[k] = lse
            total = total + jnp.sum(lse - target, axis=1, keepdims=True)
        loss_ref[...] = jnp.broadcast_to(total / (n * t), loss_ref.shape)


def stat_sum(n, me, own, parts):
    total = None
    for a in range(n):
        r = lax.rem(me - a + n, n)
        term = own
        for k in range(1, n):
            term = jnp.where(r == k, parts[k - 1], term)
        total = term if total is None else total + term
    return total


def run_stats(n, tile, hidden, targets, w_blk, collective_id):
    tok, d = hidden.shape
    vocab = w_blk.shape[0]
    t = tok // n
    return pl.pallas_call(
        functools.partial(stats_kernel, n, tile),
        grid=(n,),
        in_specs=[
            pl.BlockSpec((t, d), lambda c: (c, 0)),
            pl.BlockSpec((vocab, d), lambda c: (0, 0), pipeline_mode=pl.Buffered(1)),
            pl.BlockSpec((n, 1, t), lambda c: (0, 0, 0)),
        ],
        out_specs=[
            pl.BlockSpec(memory_space=pl.ANY),
            pl.BlockSpec((n, 1, t), lambda c: (0, 0, 0)),
            pl.BlockSpec((8, 128), lambda c: (0, 0)),
        ],
        out_shape=[
            jax.ShapeDtypeStruct((n, vocab, t), jnp.float32),
            jax.ShapeDtypeStruct((n, 1, t), jnp.float32),
            jax.ShapeDtypeStruct((8, 128), jnp.float32),
        ],
        scratch_shapes=[
            pltpu.VMEM((2, vocab, t), jnp.float32),
            pltpu.VMEM((n, 8, t), jnp.float32),
            pltpu.VMEM((n, n - 1, 8, t), jnp.float32),
            pltpu.SemaphoreType.DMA((2,)),
            pltpu.SemaphoreType.DMA,
            pltpu.SemaphoreType.DMA,
        ],
        compiler_params=pltpu.CompilerParams(
            dimension_semantics=("arbitrary",),
            collective_id=collective_id,
            has_side_effects=True,
            vmem_limit_bytes=VMEM_LIMIT,
        ),
        name="stats",
    )(hidden, w_blk, targets)


def hidden_grad_kernel(
    n, tile, w_hbm, z_hbm, lse_ref, tgt_ref, dht_ref, dz_hbm,
    w, zin, dz, hacc, from_partner, from_ring,
    wsem, zsem, dzsem, p_send, p_recv, r_send, r_recv,
):
    me = lax.axis_index(AXIS)
    nx = n // 2
    x, core = lax.div(me, 2), lax.rem(me, 2)
    sgn = 1 - 2 * core
    d, t = dht_ref.shape
    vocab = w.shape[0]
    tiles = blocks_of(0, vocab, tile)
    last = len(tiles) - 1
    partner = 2 * x + (1 - core)
    ahead = 2 * lax.rem(x + sgn + nx, nx) + core
    behind = 2 * lax.rem(x - sgn + nx, nx) + core

    def chunk_of(s):
        q, mine = lax.div(s, 2), lax.rem(s, 2)
        e = sgn * (2 * mine - 1)
        off = jnp.where(q == 0, 2, jnp.where(q == 1, e, jnp.where(q == 2, -e, 0)))
        owner_core = core * mine + (1 - core) * (1 - mine)
        return 2 * lax.rem(x + off + nx, nx) + owner_core

    def z_copy(chunk, j):
        r0, rows = tiles[j]
        return pltpu.make_async_copy(
            z_hbm.at[chunk, pl.ds(r0, rows)], zin.at[j % 3, pl.ds(0, rows)], zsem.at[j % 3]
        )

    def dz_copy(chunk, j):
        r0, rows = tiles[j]
        return pltpu.make_async_copy(
            dz.at[j % 3, pl.ds(0, rows)],
            dz_hbm.at[pl.ds(r0, rows), pl.ds(pl.multiple_of(chunk * t, t), t)],
            dzsem.at[j % 3],
        )

    def partner_copy(q):
        return pltpu.make_async_remote_copy(
            src_ref=hacc.at[0], dst_ref=from_partner.at[q], send_sem=p_send.at[q], recv_sem=p_recv.at[q],
            device_id={AXIS: partner}, device_id_type=MESH,
        )

    def ring_copy(q, peer):
        return pltpu.make_async_remote_copy(
            src_ref=hacc.at[1 + lax.rem(q, 2)], dst_ref=from_ring.at[q], send_sem=r_send.at[q], recv_sem=r_recv.at[q],
            device_id={AXIS: peer}, device_id_type=MESH,
        )

    first = chunk_of(0)
    w_copy = pltpu.make_async_copy(w_hbm, w, wsem)
    for j in range(3):
        z_copy(first, j).start()
    w_copy.start()

    barrier = pltpu.get_barrier_semaphore()
    for peer in (partner, ahead, behind):
        pl.semaphore_signal(barrier, inc=1, device_id={AXIS: peer}, device_id_type=MESH)
    pl.semaphore_wait(barrier, 3)
    w_copy.wait()

    def stage(s, carry):
        chunk, following = chunk_of(s), chunk_of(jnp.minimum(s + 1, n - 1))
        q, mine = lax.div(s, 2), lax.rem(s, 2)
        acc = mine * (1 + lax.rem(q, 2))
        pq, pmine = lax.div(s - 1, 2), lax.rem(s + 1, 2)
        pacc = 1 + lax.rem(pq, 2)
        lse, tgt = lse_ref[chunk], tgt_ref[chunk] - me * vocab

        @pl.when(jnp.logical_and(mine == 0, q >= 1))
        def _():
            partner_copy(q - 1).wait_send()

        @pl.when(jnp.logical_and(mine == 1, q >= 2))
        def _():
            ring_copy(q - 2, ahead).wait_send()

        for j, (r0, rows) in enumerate(tiles):
            z_copy(chunk, j).wait()
            if j < 3:

                @pl.when(s >= 1)
                def _():
                    dz_copy(chunk, j + last - 2).wait()

            else:
                dz_copy(chunk, j - 3).wait()
            parts = []
            for b0, size in blocks_of(0, rows, PIECE):
                z = zin[j % 3, b0 : b0 + size, :]
                hit = lax.broadcasted_iota(jnp.int32, (size, t), 0) == tgt - (r0 + b0)
                g = (jnp.exp(z - lse) - jnp.where(hit, 1.0, 0.0)) * (1.0 / (n * t))
                g = g.astype(jnp.bfloat16)
                dz[j % 3, b0 : b0 + size, :] = g
                parts.append(g)
            part = lax.dot_general(
                w[r0 : r0 + rows, :],
                jnp.concatenate(parts, axis=0),
                (((0,), (0,)), ((), ())),
                preferred_element_type=jnp.float32,
            )
            if j == 0:
                hacc[acc] = part
            else:
                hacc[acc] = hacc[acc] + part
            dz_copy(chunk, j).start()

            if j + 3 <= last:
                z_copy(chunk, j + 3).start()
            else:

                @pl.when(s < n - 1)
                def _():
                    z_copy(following, j + 2 - last).start()

            if j == 0:

                @pl.when(jnp.logical_and(s >= 1, pmine == 1))
                def _():
                    partner_copy(pq).wait_recv()
                    hacc[pacc] = hacc[pacc] + from_partner[pq]

                    @pl.when(pq == 1)
                    def _():
                        ring_copy(0, ahead).wait_recv()
                        hacc[pacc] = hacc[pacc] + from_ring[0]

            if j == 1:

                @pl.when(jnp.logical_and(s >= 1, pmine == 0))
                def _():
                    partner_copy(pq).start()

                @pl.when(jnp.logical_and(s >= 1, jnp.logical_and(pmine == 1, pq < 2)))
                def _():
                    ring_copy(pq, ahead).start()

                @pl.when(jnp.logical_and(s >= 1, jnp.logical_and(pmine == 1, pq == 2)))
                def _():
                    ring_copy(2, behind).start()

        return carry

    lax.fori_loop(0, n, stage, 0)

    for j in range(last - 2, last + 1):
        dz_copy(chunk_of(n - 1), j).wait()
    partner_copy(3).wait_recv()
    total = hacc[2] + from_partner[3]
    ring_copy(1, ahead).wait_recv()
    total = total + from_ring[1]
    ring_copy(2, behind).wait_recv()
    dht_ref[...] = total + from_ring[2]
    partner_copy(3).wait_send()
    ring_copy(2, behind).wait_send()


def run_hidden_grad(n, tile, w_blk, z, lse, targets, collective_id):
    vocab, d = w_blk.shape
    t = z.shape[2]
    rows = blocks_of(0, vocab, tile)[-1][1]
    any_spec = pl.BlockSpec(memory_space=pl.ANY)
    vmem_spec = pl.BlockSpec(memory_space=pltpu.VMEM)
    return pl.pallas_call(
        functools.partial(hidden_grad_kernel, n, tile),
        in_specs=[any_spec, any_spec, vmem_spec, vmem_spec],
        out_specs=[vmem_spec, any_spec],
        out_shape=[
            jax.ShapeDtypeStruct((d, t), jnp.float32),
            jax.ShapeDtypeStruct((vocab, n * t), jnp.bfloat16),
        ],
        scratch_shapes=[
            pltpu.VMEM((vocab, d), jnp.bfloat16),
            pltpu.VMEM((3, rows, t), jnp.float32),
            pltpu.VMEM((3, rows, t), jnp.bfloat16),
            pltpu.VMEM((3, d, t), jnp.float32),
            pltpu.VMEM((4, d, t), jnp.float32),
            pltpu.VMEM((3, d, t), jnp.float32),
            pltpu.SemaphoreType.DMA,
            pltpu.SemaphoreType.DMA((3,)),
            pltpu.SemaphoreType.DMA((3,)),
            pltpu.SemaphoreType.DMA((4,)),
            pltpu.SemaphoreType.DMA((4,)),
            pltpu.SemaphoreType.DMA((3,)),
            pltpu.SemaphoreType.DMA((3,)),
        ],
        compiler_params=pltpu.CompilerParams(
            collective_id=collective_id, has_side_effects=True, vmem_limit_bytes=VMEM_LIMIT
        ),
        name="hidden_grad",
    )(w_blk, z, lse, targets)


def weight_grad_kernel(dz_ref, h_ref, dw_ref):
    dw_ref[...] = jnp.dot(dz_ref[...], h_ref[...], preferred_element_type=jnp.float32)


def run_weight_grad(dz, hidden):
    vocab, tok = dz.shape
    d = hidden.shape[1]
    rows = min(ROWS, vocab)
    return pl.pallas_call(
        weight_grad_kernel,
        grid=(pl.cdiv(vocab, rows),),
        in_specs=[
            pl.BlockSpec((rows, tok), lambda i: (i, 0)),
            pl.BlockSpec((tok, d), lambda i: (0, 0), pipeline_mode=pl.Buffered(1)),
        ],
        out_specs=pl.BlockSpec((rows, d), lambda i: (i, 0)),
        out_shape=jax.ShapeDtypeStruct((vocab, d), jnp.float32),
        compiler_params=pltpu.CompilerParams(dimension_semantics=("arbitrary",), vmem_limit_bytes=VMEM_LIMIT),
        name="weight_grad",
    )(dz, hidden)


def solution(mesh, tile=TILE):
    n = mesh.shape[AXIS]

    def local_step(hidden, targets, w_blk):
        tgt = targets.reshape(n, 1, hidden.shape[0] // n)
        z, lse, loss = run_stats(n, tile, hidden, tgt, w_blk, 0)
        dht, dz = run_hidden_grad(n, tile, w_blk, z, lse, tgt, 1)
        return loss[0, :1], dht.T, run_weight_grad(dz, hidden)

    return jax.shard_map(
        local_step,
        mesh=mesh,
        in_specs=(P("data", None), P("data"), P(AXIS, None)),
        out_specs=(P("data"), P(("data", AXIS), None), P(("data", AXIS), None)),
        check_vma=False,
    )
```

```python
import functools

import jax
import jax.numpy as jnp
from jax import lax
from jax.experimental import pallas as pl
from jax.experimental.pallas import tpu as pltpu
from jax.sharding import PartitionSpec as P

MESH = pl.DeviceIdType.MESH
AXIS = "fsdp"
TILE = 1024
PIECE = 256
ROWS = 528
VMEM_LIMIT = 67043328


def blocks_of(start, count, size):
    blocks = max(count // size, 1)
    return [(start + i * size, size if i < blocks - 1 else count - i * size) for i in range(blocks)]


def stats_kernel(
    n, tile, h_ref, w_hbm, tgt_ref, z_hbm, lse_ref, loss_ref, w_ref, zbuf, stat, recv, wsem, zsem, send_sem, recv_sem
):
    c = pl.program_id(0)
    p = lax.rem(c, 2)
    me = lax.axis_index(AXIS)
    vocab, t = w_ref.shape[0], h_ref.shape[0]

    halves = blocks_of(0, vocab, -(-vocab // (2 * PIECE)) * PIECE)

    def w_copy(i):
        r0, rows = halves[i]
        return pltpu.make_async_copy(w_hbm.at[pl.ds(r0, rows)], w_ref.at[pl.ds(r0, rows)], wsem.at[i])

    @pl.when(c == 0)
    def _():
        for i in range(len(halves)):
            w_copy(i).start()
        barrier = pltpu.get_barrier_semaphore()
        for r in range(1, n):
            pl.semaphore_signal(barrier, inc=1, device_id={AXIS: lax.rem(me + r, n)}, device_id_type=MESH)
        pl.semaphore_wait(barrier, n - 1)
        stat[...] = jnp.zeros_like(stat)
        w_copy(0).wait()

    def send(chunk):
        for r in range(1, n):
            pltpu.make_async_remote_copy(
                src_ref=stat.at[chunk],
                dst_ref=recv.at[chunk, r - 1],
                send_sem=send_sem,
                recv_sem=recv_sem,
                device_id={AXIS: lax.rem(me + r, n)},
                device_id_type=MESH,
            ).start()

    @pl.when(c >= 1)
    def _():
        send(c - 1)

    @pl.when(c >= 2)
    def _():
        pltpu.make_async_copy(zbuf.at[p], z_hbm.at[c - 2], zsem.at[p]).wait()

    tgt = tgt_ref[c] - me * vocab
    maxima, totals, hits = [], [], []
    for r0, rows in blocks_of(0, vocab, PIECE):
        if len(halves) > 1 and r0 == halves[1][0]:

            @pl.when(c == 0)
            def _():
                w_copy(1).wait()

        z = lax.dot_general(
            w_ref[r0 : r0 + rows, :], h_ref[...], (((1,), (1,)), ((), ())), preferred_element_type=jnp.float32
        )
        zbuf[p, r0 : r0 + rows, :] = z
        big = jnp.max(z, axis=0, keepdims=True)
        total = jnp.sum(jnp.exp(z - big), axis=0, keepdims=True)
        hit = lax.broadcasted_iota(jnp.int32, (rows, t), 0) == tgt - r0
        maxima.append(big)
        totals.append(total)
        hits.append(jnp.sum(jnp.where(hit, z, 0.0), axis=0, keepdims=True))
    for r0, rows in blocks_of(0, vocab, tile):
        pltpu.make_async_copy(zbuf.at[p, pl.ds(r0, rows)], z_hbm.at[c, pl.ds(r0, rows)], zsem.at[p]).start()
    m = functools.reduce(jnp.maximum, maxima)
    stat[c, 0:1, :] = m
    stat[c, 1:2, :] = sum(s * jnp.exp(big - m) for s, big in zip(totals, maxima))
    stat[c, 2:3, :] = sum(hits)

    @pl.when(c == n - 1)
    def _():
        send(c)
        pltpu.make_async_copy(zbuf.at[1 - p], z_hbm.at[c - 1], zsem.at[1 - p]).wait()
        pltpu.make_async_copy(zbuf.at[p], z_hbm.at[c], zsem.at[p]).wait()
        pltpu.make_async_copy(recv, recv, send_sem).wait()
        pltpu.make_async_copy(recv, recv, recv_sem).wait()
        total = jnp.float32(0.0)
        for k in range(n):
            big = stat[k, 0:1, :]
            for r in range(n - 1):
                big = jnp.maximum(big, recv[k, r, 0:1, :])
            own = stat[k, 1:2, :] * jnp.exp(stat[k, 0:1, :] - big)
            parts = [recv[k, r, 1:2, :] * jnp.exp(recv[k, r, 0:1, :] - big) for r in range(n - 1)]
            sums = stat_sum(n, me, own, parts)
            target = stat[k, 2:3, :]
            for r in range(n - 1):
                target = target + recv[k, r, 2:3, :]
            lse = big + jnp.log(sums)
            lse_ref[k] = lse
            total = total + jnp.sum(lse - target)
        loss_ref[0] = total * (1.0 / (n * t))


def stat_sum(n, me, own, parts):
    total = None
    for a in range(n):
        r = lax.rem(me - a + n, n)
        term = own
        for k in range(1, n):
            term = jnp.where(r == k, parts[k - 1], term)
        total = term if total is None else total + term
    return total


def run_stats(n, tile, hidden, targets, w_blk, collective_id):
    tok, d = hidden.shape
    vocab = w_blk.shape[0]
    t = tok // n
    return pl.pallas_call(
        functools.partial(stats_kernel, n, tile),
        grid=(n,),
        in_specs=[
            pl.BlockSpec((t, d), lambda c: (c, 0)),
            pl.BlockSpec(memory_space=pl.ANY),
            pl.BlockSpec((n, 1, t), lambda c: (0, 0, 0)),
        ],
        out_specs=[
            pl.BlockSpec(memory_space=pl.ANY),
            pl.BlockSpec((n, 1, t), lambda c: (0, 0, 0)),
            pl.BlockSpec(memory_space=pltpu.SMEM),
        ],
        out_shape=[
            jax.ShapeDtypeStruct((n, vocab, t), jnp.float32),
            jax.ShapeDtypeStruct((n, 1, t), jnp.float32),
            jax.ShapeDtypeStruct((1,), jnp.float32),
        ],
        scratch_shapes=[
            pltpu.VMEM((vocab, d), jnp.bfloat16),
            pltpu.VMEM((2, vocab, t), jnp.float32),
            pltpu.VMEM((n, 8, t), jnp.float32),
            pltpu.VMEM((n, n - 1, 8, t), jnp.float32),
            pltpu.SemaphoreType.DMA((2,)),
            pltpu.SemaphoreType.DMA((2,)),
            pltpu.SemaphoreType.DMA,
            pltpu.SemaphoreType.DMA,
        ],
        compiler_params=pltpu.CompilerParams(
            dimension_semantics=("arbitrary",),
            collective_id=collective_id,
            has_side_effects=True,
            vmem_limit_bytes=VMEM_LIMIT,
        ),
        name="stats",
    )(hidden, w_blk, targets)


def hidden_grad_kernel(
    n, tile, rows_w, blocks_w, w_hbm, z_hbm, h_hbm, lse_ref, tgt_ref, dht_ref, dz_hbm, dw_hbm,
    w, zin, dz, hacc, from_partner, from_ring, h, dzb, dwb,
    wsem, zsem, dzsem, p_send, p_recv, r_send, r_recv, hsem, bsem, dwsem,
):
    me = lax.axis_index(AXIS)
    nx = n // 2
    x, core = lax.div(me, 2), lax.rem(me, 2)
    sgn = 1 - 2 * core
    d, t = dht_ref.shape
    vocab = w.shape[0]
    tiles = blocks_of(0, vocab, tile)
    last = len(tiles) - 1
    partner = 2 * x + (1 - core)
    ahead = 2 * lax.rem(x + sgn + nx, nx) + core
    behind = 2 * lax.rem(x - sgn + nx, nx) + core

    def chunk_of(s):
        q, mine = lax.div(s, 2), lax.rem(s, 2)
        e = sgn * (2 * mine - 1)
        off = jnp.where(q == 0, 2, jnp.where(q == 1, e, jnp.where(q == 2, -e, 0)))
        owner_core = core * mine + (1 - core) * (1 - mine)
        return 2 * lax.rem(x + off + nx, nx) + owner_core

    def z_copy(chunk, j):
        r0, rows = tiles[j]
        return pltpu.make_async_copy(
            z_hbm.at[chunk, pl.ds(r0, rows)], zin.at[j % 3, pl.ds(0, rows)], zsem.at[j % 3]
        )

    def dz_copy(chunk, j):
        r0, rows = tiles[j]
        return pltpu.make_async_copy(
            dz.at[j % 3, pl.ds(0, rows)],
            dz_hbm.at[pl.ds(r0, rows), pl.ds(pl.multiple_of(chunk * t, t), t)],
            dzsem.at[j % 3],
        )

    def partner_copy(q):
        return pltpu.make_async_remote_copy(
            src_ref=hacc.at[0], dst_ref=from_partner.at[q], send_sem=p_send.at[q], recv_sem=p_recv.at[q],
            device_id={AXIS: partner}, device_id_type=MESH,
        )

    def ring_copy(q, peer):
        return pltpu.make_async_remote_copy(
            src_ref=hacc.at[1 + lax.rem(q, 2)], dst_ref=from_ring.at[q], send_sem=r_send.at[q], recv_sem=r_recv.at[q],
            device_id={AXIS: peer}, device_id_type=MESH,
        )

    def block_copy(i):
        return pltpu.make_async_copy(
            dz_hbm.at[pl.ds(i * rows_w, rows_w)], dzb.at[lax.rem(i, 2)], bsem.at[lax.rem(i, 2)]
        )

    def dw_copy(i):
        return pltpu.make_async_copy(
            dwb.at[lax.rem(i, 2)], dw_hbm.at[pl.ds(i * rows_w, rows_w)], dwsem.at[lax.rem(i, 2)]
        )

    h_copy = pltpu.make_async_copy(h_hbm, h, hsem)
    first = chunk_of(0)
    w_copy = pltpu.make_async_copy(w_hbm, w, wsem)
    for j in range(3):
        z_copy(first, j).start()
    w_copy.start()

    barrier = pltpu.get_barrier_semaphore()
    for peer in (partner, ahead, behind):
        pl.semaphore_signal(barrier, inc=1, device_id={AXIS: peer}, device_id_type=MESH)
    pl.semaphore_wait(barrier, 3)
    w_copy.wait()
    h_copy.start()

    def stage(s, carry):
        chunk, following = chunk_of(s), chunk_of(jnp.minimum(s + 1, n - 1))
        q, mine = lax.div(s, 2), lax.rem(s, 2)
        acc = mine * (1 + lax.rem(q, 2))
        pq, pmine = lax.div(s - 1, 2), lax.rem(s + 1, 2)
        pacc = 1 + lax.rem(pq, 2)
        lse, tgt = lse_ref[chunk], tgt_ref[chunk] - me * vocab

        @pl.when(jnp.logical_and(mine == 0, q >= 1))
        def _():
            partner_copy(q - 1).wait_send()

        @pl.when(jnp.logical_and(mine == 1, q >= 2))
        def _():
            ring_copy(q - 2, ahead).wait_send()

        for j, (r0, rows) in enumerate(tiles):
            z_copy(chunk, j).wait()
            if j < 3:

                @pl.when(s >= 1)
                def _():
                    dz_copy(chunk, j + last - 2).wait()

            else:
                dz_copy(chunk, j - 3).wait()
                if j == 3:

                    @pl.when(s == n - 1)
                    def _():
                        block_copy(0).start()

            parts = []
            for b0, size in blocks_of(0, rows, PIECE):
                z = zin[j % 3, b0 : b0 + size, :]
                hit = lax.broadcasted_iota(jnp.int32, (size, t), 0) == tgt - (r0 + b0)
                g = (jnp.exp(z - lse) - jnp.where(hit, 1.0, 0.0)) * (1.0 / (n * t))
                g = g.astype(jnp.bfloat16)
                dz[j % 3, b0 : b0 + size, :] = g
                parts.append(g)
            part = lax.dot_general(
                w[r0 : r0 + rows, :],
                jnp.concatenate(parts, axis=0),
                (((0,), (0,)), ((), ())),
                preferred_element_type=jnp.float32,
            )
            if j == 0:
                hacc[acc] = part
            else:
                hacc[acc] = hacc[acc] + part
            dz_copy(chunk, j).start()

            if j + 3 <= last:
                z_copy(chunk, j + 3).start()
            else:

                @pl.when(s < n - 1)
                def _():
                    z_copy(following, j + 2 - last).start()

            if j == 0:

                @pl.when(jnp.logical_and(s >= 1, pmine == 1))
                def _():
                    partner_copy(pq).wait_recv()
                    hacc[pacc] = hacc[pacc] + from_partner[pq]

                @pl.when(s == 5)
                def _():
                    ring_copy(0, ahead).wait_recv()
                    hacc[2] = hacc[2] + from_ring[0]

            if j == 1:

                @pl.when(jnp.logical_and(s >= 1, pmine == 0))
                def _():
                    partner_copy(pq).start()

                @pl.when(s == 2)
                def _():
                    ring_copy(0, ahead).start()

                @pl.when(s == 5)
                def _():
                    ring_copy(1, ahead).start()

                @pl.when(s == 6)
                def _():
                    ring_copy(2, behind).start()

        return carry

    lax.fori_loop(0, n, stage, 0)

    for j in range(last - 2, last + 1):
        dz_copy(chunk_of(n - 1), j).wait()
    h_copy.wait()

    def block(i, carry):
        slot = lax.rem(i, 2)

        @pl.when(i + 1 < blocks_w)
        def _():
            block_copy(i + 1).start()

        @pl.when(i >= 2)
        def _():
            dw_copy(i - 2).wait()

        block_copy(i).wait()
        dwb[slot] = jnp.dot(dzb[slot], h[...], preferred_element_type=jnp.float32)
        dw_copy(i).start()
        return carry

    lax.fori_loop(0, blocks_w, block, 0)
    partner_copy(3).wait_recv()
    total = hacc[2] + from_partner[3]
    ring_copy(1, ahead).wait_recv()
    total = total + from_ring[1]
    ring_copy(2, behind).wait_recv()
    dht_ref[...] = total + from_ring[2]
    partner_copy(3).wait_send()
    ring_copy(2, behind).wait_send()
    for i in range(max(blocks_w - 2, 0), blocks_w):
        dw_copy(i).wait()


def run_hidden_grad(n, tile, rows_w, blocks_w, w_blk, z, hidden, lse, targets, collective_id):
    vocab, d = w_blk.shape
    t = z.shape[2]
    rows = blocks_of(0, vocab, tile)[-1][1]
    any_spec = pl.BlockSpec(memory_space=pl.ANY)
    vmem_spec = pl.BlockSpec(memory_space=pltpu.VMEM)
    return pl.pallas_call(
        functools.partial(hidden_grad_kernel, n, tile, rows_w, blocks_w),
        in_specs=[any_spec, any_spec, any_spec, vmem_spec, vmem_spec],
        out_specs=[vmem_spec, any_spec, any_spec],
        out_shape=[
            jax.ShapeDtypeStruct((d, t), jnp.float32),
            jax.ShapeDtypeStruct((vocab, n * t), jnp.bfloat16),
            jax.ShapeDtypeStruct((blocks_w * rows_w, d), jnp.float32),
        ],
        scratch_shapes=[
            pltpu.VMEM((vocab, d), jnp.bfloat16),
            pltpu.VMEM((3, rows, t), jnp.float32),
            pltpu.VMEM((3, rows, t), jnp.bfloat16),
            pltpu.VMEM((3, d, t), jnp.float32),
            pltpu.VMEM((4, d, t), jnp.float32),
            pltpu.VMEM((3, d, t), jnp.float32),
            pltpu.VMEM((n * t, d), jnp.bfloat16),
            pltpu.VMEM((2, rows_w, n * t), jnp.bfloat16),
            pltpu.VMEM((2, rows_w, d), jnp.float32),
            pltpu.SemaphoreType.DMA,
            pltpu.SemaphoreType.DMA((3,)),
            pltpu.SemaphoreType.DMA((3,)),
            pltpu.SemaphoreType.DMA((4,)),
            pltpu.SemaphoreType.DMA((4,)),
            pltpu.SemaphoreType.DMA((3,)),
            pltpu.SemaphoreType.DMA((3,)),
            pltpu.SemaphoreType.DMA,
            pltpu.SemaphoreType.DMA((2,)),
            pltpu.SemaphoreType.DMA((2,)),
        ],
        compiler_params=pltpu.CompilerParams(
            collective_id=collective_id, has_side_effects=True, vmem_limit_bytes=VMEM_LIMIT
        ),
        name="hidden_grad",
    )(w_blk, z, hidden, lse, targets)


def weight_grad_kernel(
    rows, done, vocab, dz_ref, h_ref, part_ref, dht_ref, loss_in, dw_hbm, dh_hbm, loss_out, buf, dh, osem, csem, hsem
):
    i = pl.program_id(0)
    steps = pl.num_programs(0)
    slot = lax.rem(i, 2)
    final = vocab - (done + steps - 1) * rows

    def out_copy(k, size):
        return pltpu.make_async_copy(
            buf.at[lax.rem(k, 2), pl.ds(0, size)], dw_hbm.at[pl.ds((done + k) * rows, size)], osem.at[lax.rem(k, 2)]
        )

    dh_copy = pltpu.make_async_copy(dh, dh_hbm, hsem)
    part_copy = pltpu.make_async_copy(part_ref, dw_hbm.at[pl.ds(i * rows, rows)], csem)

    @pl.when(i < done)
    def _():
        part_copy.start()

    @pl.when(i == 0)
    def _():
        loss_out[0] = loss_in[0]
        dh[...] = dht_ref[...].T
        dh_copy.start()

    @pl.when(i >= 2)
    def _():
        out_copy(i - 2, rows).wait()

    buf[slot] = jnp.dot(dz_ref[...], h_ref[...], preferred_element_type=jnp.float32)

    @pl.when(i < done)
    def _():
        part_copy.wait()

    @pl.when(i < steps - 1)
    def _():
        out_copy(i, rows).start()

    @pl.when(i == steps - 1)
    def _():
        out_copy(i, final).start()
        out_copy(i - 1, rows).wait()
        out_copy(i, final).wait()
        dh_copy.wait()


def run_weight_grad(rows, done, dz, hidden, part, dht, loss):
    vocab, tok = dz.shape
    d, t = dht.shape
    steps = pl.cdiv(vocab, rows) - done
    assert done <= steps and steps >= 2
    any_spec = pl.BlockSpec(memory_space=pl.ANY)
    smem_spec = pl.BlockSpec(memory_space=pltpu.SMEM)
    return pl.pallas_call(
        functools.partial(weight_grad_kernel, rows, done, vocab),
        grid=(steps,),
        in_specs=[
            pl.BlockSpec((rows, tok), lambda i: (done + i, 0)),
            pl.BlockSpec((tok, d), lambda i: (0, 0), pipeline_mode=pl.Buffered(1)),
            pl.BlockSpec((rows, d), lambda i: (jnp.minimum(i, done - 1), 0)),
            pl.BlockSpec((d, t), lambda i: (0, 0), pipeline_mode=pl.Buffered(1)),
            smem_spec,
        ],
        out_specs=[any_spec, any_spec, smem_spec],
        out_shape=[
            jax.ShapeDtypeStruct((vocab, d), jnp.float32),
            jax.ShapeDtypeStruct((t, d), jnp.float32),
            jax.ShapeDtypeStruct((1,), jnp.float32),
        ],
        scratch_shapes=[
            pltpu.VMEM((2, rows, d), jnp.float32),
            pltpu.VMEM((t, d), jnp.float32),
            pltpu.SemaphoreType.DMA((2,)),
            pltpu.SemaphoreType.DMA,
            pltpu.SemaphoreType.DMA,
        ],
        compiler_params=pltpu.CompilerParams(dimension_semantics=("arbitrary",), vmem_limit_bytes=VMEM_LIMIT),
        name="weight_grad",
    )(dz, hidden, part, dht, loss)


def solution(mesh, tile=TILE, rows_w=ROWS):
    n = mesh.shape[AXIS]

    def local_step(hidden, targets, w_blk):
        tgt = targets.reshape(n, 1, hidden.shape[0] // n)
        z, lse, loss = run_stats(n, tile, hidden, tgt, w_blk, 0)
        done = pl.cdiv(w_blk.shape[0], rows_w) // 2
        dht, dz, part = run_hidden_grad(n, tile, rows_w, done, w_blk, z, hidden, lse, tgt, 1)
        dw, dh, loss = run_weight_grad(rows_w, done, dz, hidden, part, dht, loss)
        return loss, dh, dw

    return jax.shard_map(
        local_step,
        mesh=mesh,
        in_specs=(P("data", None), P("data"), P(AXIS, None)),
        out_specs=(P("data"), P(("data", AXIS), None), P(("data", AXIS), None)),
        check_vma=False,
    )
```

```python
import functools

import jax
import jax.numpy as jnp
from jax import lax
from jax.experimental import pallas as pl
from jax.experimental.pallas import tpu as pltpu
from jax.sharding import PartitionSpec as P

MESH = pl.DeviceIdType.MESH
AXIS = "fsdp"
TILE = 1024
PIECE = 256
ROWS = 528
VMEM_LIMIT = 67043328


def blocks_of(start, count, size):
    blocks = max(count // size, 1)
    return [(start + i * size, size if i < blocks - 1 else count - i * size) for i in range(blocks)]


def stats_kernel(
    n, tile, h_ref, w_hbm, tgt_ref, z_hbm, lse_ref, loss_ref, w_ref, zbuf, stat, recv, wsem, zsem, send_sem, recv_sem
):
    c = pl.program_id(0)
    p = lax.rem(c, 2)
    me = lax.axis_index(AXIS)
    vocab, t = w_ref.shape[0], h_ref.shape[0]

    halves = blocks_of(0, vocab, -(-vocab // (2 * PIECE)) * PIECE)

    def w_copy(i):
        r0, rows = halves[i]
        return pltpu.make_async_copy(w_hbm.at[pl.ds(r0, rows)], w_ref.at[pl.ds(r0, rows)], wsem.at[i])

    @pl.when(c == 0)
    def _():
        for i in range(len(halves)):
            w_copy(i).start()
        barrier = pltpu.get_barrier_semaphore()
        for r in range(1, n):
            pl.semaphore_signal(barrier, inc=1, device_id={AXIS: lax.rem(me + r, n)}, device_id_type=MESH)
        pl.semaphore_wait(barrier, n - 1)
        stat[...] = jnp.zeros_like(stat)
        w_copy(0).wait()

    def send(chunk):
        for r in range(1, n):
            pltpu.make_async_remote_copy(
                src_ref=stat.at[chunk],
                dst_ref=recv.at[chunk, r - 1],
                send_sem=send_sem,
                recv_sem=recv_sem,
                device_id={AXIS: lax.rem(me + r, n)},
                device_id_type=MESH,
            ).start()

    @pl.when(c >= 1)
    def _():
        send(c - 1)

    @pl.when(c >= 2)
    def _():
        pltpu.make_async_copy(zbuf.at[p], z_hbm.at[c - 2], zsem.at[p]).wait()

    tgt = tgt_ref[c] - me * vocab
    maxima, totals, hits = [], [], []
    for r0, rows in blocks_of(0, vocab, PIECE):
        if len(halves) > 1 and r0 == halves[1][0]:

            @pl.when(c == 0)
            def _():
                w_copy(1).wait()

        z = lax.dot_general(
            w_ref[r0 : r0 + rows, :], h_ref[...], (((1,), (1,)), ((), ())), preferred_element_type=jnp.float32
        )
        zbuf[p, r0 : r0 + rows, :] = z
        big = jnp.max(z, axis=0, keepdims=True)
        total = jnp.sum(jnp.exp(z - big), axis=0, keepdims=True)
        hit = lax.broadcasted_iota(jnp.int32, (rows, t), 0) == tgt - r0
        maxima.append(big)
        totals.append(total)
        hits.append(jnp.sum(jnp.where(hit, z, 0.0), axis=0, keepdims=True))
    for r0, rows in blocks_of(0, vocab, tile):
        pltpu.make_async_copy(zbuf.at[p, pl.ds(r0, rows)], z_hbm.at[c, pl.ds(r0, rows)], zsem.at[p]).start()
    m = functools.reduce(jnp.maximum, maxima)
    stat[c, 0:1, :] = m
    stat[c, 1:2, :] = sum(s * jnp.exp(big - m) for s, big in zip(totals, maxima))
    stat[c, 2:3, :] = sum(hits)

    @pl.when(c == n - 1)
    def _():
        send(c)
        pltpu.make_async_copy(recv, recv, recv_sem).wait()
        total = jnp.float32(0.0)
        for k in range(n):
            big = stat[k, 0:1, :]
            for r in range(n - 1):
                big = jnp.maximum(big, recv[k, r, 0:1, :])
            own = stat[k, 1:2, :] * jnp.exp(stat[k, 0:1, :] - big)
            parts = [recv[k, r, 1:2, :] * jnp.exp(recv[k, r, 0:1, :] - big) for r in range(n - 1)]
            sums = stat_sum(n, me, own, parts)
            target = stat[k, 2:3, :]
            for r in range(n - 1):
                target = target + recv[k, r, 2:3, :]
            lse = big + jnp.log(sums)
            lse_ref[k] = lse
            total = total + jnp.sum(lse - target)
        loss_ref[0] = total * (1.0 / (n * t))
        pltpu.make_async_copy(recv, recv, send_sem).wait()
        pltpu.make_async_copy(zbuf.at[1 - p], z_hbm.at[c - 1], zsem.at[1 - p]).wait()
        pltpu.make_async_copy(zbuf.at[p], z_hbm.at[c], zsem.at[p]).wait()


def stat_sum(n, me, own, parts):
    total = None
    for a in range(n):
        r = lax.rem(me - a + n, n)
        term = own
        for k in range(1, n):
            term = jnp.where(r == k, parts[k - 1], term)
        total = term if total is None else total + term
    return total


def run_stats(n, tile, hidden, targets, w_blk, collective_id):
    tok, d = hidden.shape
    vocab = w_blk.shape[0]
    t = tok // n
    return pl.pallas_call(
        functools.partial(stats_kernel, n, tile),
        grid=(n,),
        in_specs=[
            pl.BlockSpec((t, d), lambda c: (c, 0)),
            pl.BlockSpec(memory_space=pl.ANY),
            pl.BlockSpec((n, 1, t), lambda c: (0, 0, 0)),
        ],
        out_specs=[
            pl.BlockSpec(memory_space=pl.ANY),
            pl.BlockSpec((n, 1, t), lambda c: (0, 0, 0)),
            pl.BlockSpec(memory_space=pltpu.SMEM),
        ],
        out_shape=[
            jax.ShapeDtypeStruct((n, vocab, t), jnp.float32),
            jax.ShapeDtypeStruct((n, 1, t), jnp.float32),
            jax.ShapeDtypeStruct((1,), jnp.float32),
        ],
        scratch_shapes=[
            pltpu.VMEM((vocab, d), jnp.bfloat16),
            pltpu.VMEM((2, vocab, t), jnp.float32),
            pltpu.VMEM((n, 8, t), jnp.float32),
            pltpu.VMEM((n, n - 1, 8, t), jnp.float32),
            pltpu.SemaphoreType.DMA((2,)),
            pltpu.SemaphoreType.DMA((2,)),
            pltpu.SemaphoreType.DMA,
            pltpu.SemaphoreType.DMA,
        ],
        compiler_params=pltpu.CompilerParams(
            dimension_semantics=("arbitrary",),
            collective_id=collective_id,
            has_side_effects=True,
            vmem_limit_bytes=VMEM_LIMIT,
        ),
        name="stats",
    )(hidden, w_blk, targets)


def hidden_grad_kernel(
    n, tile, rows_w, blocks_w, w_hbm, z_hbm, h_hbm, lse_ref, tgt_ref, dht_ref, dz_hbm, dw_hbm,
    w, zin, dz, hacc, from_partner, from_ring, h, dzb, dwb,
    wsem, zsem, dzsem, p_send, p_recv, r_send, r_recv, hsem, bsem, dwsem,
):
    me = lax.axis_index(AXIS)
    nx = n // 2
    x, core = lax.div(me, 2), lax.rem(me, 2)
    sgn = 1 - 2 * core
    d, t = dht_ref.shape
    vocab = w.shape[0]
    tiles = blocks_of(0, vocab, tile)
    last = len(tiles) - 1
    partner = 2 * x + (1 - core)
    ahead = 2 * lax.rem(x + sgn + nx, nx) + core
    behind = 2 * lax.rem(x - sgn + nx, nx) + core

    def chunk_of(s):
        q, mine = lax.div(s, 2), lax.rem(s, 2)
        e = sgn * (1 - 2 * mine)
        off = jnp.where(q == 0, 2, jnp.where(q == 1, e, jnp.where(q == 2, -e, 0)))
        owner_core = core * mine + (1 - core) * (1 - mine)
        return 2 * lax.rem(x + off + nx, nx) + owner_core

    def z_copy(chunk, j):
        r0, rows = tiles[j]
        return pltpu.make_async_copy(
            z_hbm.at[chunk, pl.ds(r0, rows)], zin.at[j % 3, pl.ds(0, rows)], zsem.at[j % 3]
        )

    def dz_copy(chunk, j):
        r0, rows = tiles[j]
        return pltpu.make_async_copy(
            dz.at[j % 3, pl.ds(0, rows)],
            dz_hbm.at[pl.ds(r0, rows), pl.ds(pl.multiple_of(chunk * t, t), t)],
            dzsem.at[j % 3],
        )

    def partner_copy(q):
        return pltpu.make_async_remote_copy(
            src_ref=hacc.at[0], dst_ref=from_partner.at[q], send_sem=p_send.at[q], recv_sem=p_recv.at[q],
            device_id={AXIS: partner}, device_id_type=MESH,
        )

    def ring_copy(q, peer):
        return pltpu.make_async_remote_copy(
            src_ref=hacc.at[1 + q], dst_ref=from_ring.at[q], send_sem=r_send.at[q], recv_sem=r_recv.at[q],
            device_id={AXIS: peer}, device_id_type=MESH,
        )

    def block_copy(i):
        return pltpu.make_async_copy(
            dz_hbm.at[pl.ds(i * rows_w, rows_w)], dzb.at[lax.rem(i, 2)], bsem.at[lax.rem(i, 2)]
        )

    def dw_copy(i):
        return pltpu.make_async_copy(
            dwb.at[lax.rem(i, 2)], dw_hbm.at[pl.ds(i * rows_w, rows_w)], dwsem.at[lax.rem(i, 2)]
        )

    h_copy = pltpu.make_async_copy(h_hbm, h, hsem)
    first = chunk_of(0)
    w_copy = pltpu.make_async_copy(w_hbm, w, wsem)
    for j in range(3):
        z_copy(first, j).start()
    w_copy.start()

    barrier = pltpu.get_barrier_semaphore()
    for peer in (partner, ahead, behind):
        pl.semaphore_signal(barrier, inc=1, device_id={AXIS: peer}, device_id_type=MESH)
    pl.semaphore_wait(barrier, 3)
    w_copy.wait()
    h_copy.start()

    def stage(s, carry):
        chunk, following = chunk_of(s), chunk_of(jnp.minimum(s + 1, n - 1))
        q, mine = lax.div(s, 2), lax.rem(s, 2)
        acc = mine * (1 + q)
        pq, pmine = lax.div(s - 1, 2), lax.rem(s + 1, 2)
        pacc = 1 + pq
        lse, tgt = lse_ref[chunk], tgt_ref[chunk] - me * vocab

        @pl.when(jnp.logical_and(mine == 0, q >= 1))
        def _():
            partner_copy(q - 1).wait_send()

        for j, (r0, rows) in enumerate(tiles):
            z_copy(chunk, j).wait()
            if j < 3:

                @pl.when(s >= 1)
                def _():
                    dz_copy(chunk, j + last - 2).wait()

            else:
                dz_copy(chunk, j - 3).wait()
                if j == 3:

                    @pl.when(s == n - 1)
                    def _():
                        block_copy(0).start()

            parts = []
            for b0, size in blocks_of(0, rows, PIECE):
                z = zin[j % 3, b0 : b0 + size, :]
                hit = lax.broadcasted_iota(jnp.int32, (size, t), 0) == tgt - (r0 + b0)
                g = (jnp.exp(z - lse) - jnp.where(hit, 1.0, 0.0)) * (1.0 / (n * t))
                g = g.astype(jnp.bfloat16)
                dz[j % 3, b0 : b0 + size, :] = g
                parts.append(g)
            part = lax.dot_general(
                w[r0 : r0 + rows, :],
                jnp.concatenate(parts, axis=0),
                (((0,), (0,)), ((), ())),
                preferred_element_type=jnp.float32,
            )
            if j == 0:
                hacc[acc] = part
            else:
                hacc[acc] = hacc[acc] + part
            dz_copy(chunk, j).start()

            if j + 3 <= last:
                z_copy(chunk, j + 3).start()
            else:

                @pl.when(s < n - 1)
                def _():
                    z_copy(following, j + 2 - last).start()

            if j == 0:

                @pl.when(jnp.logical_and(s >= 1, pmine == 1))
                def _():
                    partner_copy(pq).wait_recv()
                    hacc[pacc] = hacc[pacc] + from_partner[pq]

                @pl.when(s == 7)
                def _():
                    ring_copy(0, ahead).wait_recv()
                    hacc[3] = hacc[3] + from_ring[0]

            if j == 1:

                @pl.when(jnp.logical_and(s >= 1, pmine == 0))
                def _():
                    partner_copy(pq).start()

                @pl.when(s == 2)
                def _():
                    ring_copy(0, ahead).start()

                @pl.when(s == 4)
                def _():
                    ring_copy(1, behind).start()

                @pl.when(s == 7)
                def _():
                    ring_copy(2, ahead).start()

        return carry

    lax.fori_loop(0, n, stage, 0)

    for j in range(last - 2, last + 1):
        dz_copy(chunk_of(n - 1), j).wait()
    h_copy.wait()

    def block(i, carry):
        slot = lax.rem(i, 2)

        @pl.when(i + 1 < blocks_w)
        def _():
            block_copy(i + 1).start()

        @pl.when(i >= 2)
        def _():
            dw_copy(i - 2).wait()

        block_copy(i).wait()
        dwb[slot] = jnp.dot(dzb[slot], h[...], preferred_element_type=jnp.float32)
        dw_copy(i).start()
        return carry

    lax.fori_loop(0, blocks_w, block, 0)
    partner_copy(3).wait_recv()
    ring_copy(1, behind).wait_recv()
    total = hacc[4] + from_partner[3] + from_ring[1]
    ring_copy(2, ahead).wait_recv()
    dht_ref[...] = total + from_ring[2]
    partner_copy(3).wait_send()
    ring_copy(0, ahead).wait_send()
    ring_copy(1, behind).wait_send()
    ring_copy(2, ahead).wait_send()
    for i in range(max(blocks_w - 2, 0), blocks_w):
        dw_copy(i).wait()


def run_hidden_grad(n, tile, rows_w, blocks_w, w_blk, z, hidden, lse, targets, collective_id):
    vocab, d = w_blk.shape
    t = z.shape[2]
    rows = blocks_of(0, vocab, tile)[-1][1]
    any_spec = pl.BlockSpec(memory_space=pl.ANY)
    vmem_spec = pl.BlockSpec(memory_space=pltpu.VMEM)
    return pl.pallas_call(
        functools.partial(hidden_grad_kernel, n, tile, rows_w, blocks_w),
        in_specs=[any_spec, any_spec, any_spec, vmem_spec, vmem_spec],
        out_specs=[vmem_spec, any_spec, any_spec],
        out_shape=[
            jax.ShapeDtypeStruct((d, t), jnp.float32),
            jax.ShapeDtypeStruct((vocab, n * t), jnp.bfloat16),
            jax.ShapeDtypeStruct((blocks_w * rows_w, d), jnp.float32),
        ],
        scratch_shapes=[
            pltpu.VMEM((vocab, d), jnp.bfloat16),
            pltpu.VMEM((3, rows, t), jnp.float32),
            pltpu.VMEM((3, rows, t), jnp.bfloat16),
            pltpu.VMEM((5, d, t), jnp.float32),
            pltpu.VMEM((4, d, t), jnp.float32),
            pltpu.VMEM((3, d, t), jnp.float32),
            pltpu.VMEM((n * t, d), jnp.bfloat16),
            pltpu.VMEM((2, rows_w, n * t), jnp.bfloat16),
            pltpu.VMEM((2, rows_w, d), jnp.float32),
            pltpu.SemaphoreType.DMA,
            pltpu.SemaphoreType.DMA((3,)),
            pltpu.SemaphoreType.DMA((3,)),
            pltpu.SemaphoreType.DMA((4,)),
            pltpu.SemaphoreType.DMA((4,)),
            pltpu.SemaphoreType.DMA((3,)),
            pltpu.SemaphoreType.DMA((3,)),
            pltpu.SemaphoreType.DMA,
            pltpu.SemaphoreType.DMA((2,)),
            pltpu.SemaphoreType.DMA((2,)),
        ],
        compiler_params=pltpu.CompilerParams(
            collective_id=collective_id, has_side_effects=True, vmem_limit_bytes=VMEM_LIMIT
        ),
        name="hidden_grad",
    )(w_blk, z, hidden, lse, targets)


def weight_grad_kernel(
    rows, done, vocab, dz_ref, h_ref, part_ref, dht_hbm, loss_in, dw_hbm, dh_hbm, loss_out,
    buf, dht, dh, osem, csem, hsem,
):
    i = pl.program_id(0)
    steps = pl.num_programs(0)
    slot = lax.rem(i, 2)
    final = vocab - (done + steps - 1) * rows

    def out_copy(k, size):
        return pltpu.make_async_copy(
            buf.at[lax.rem(k, 2), pl.ds(0, size)], dw_hbm.at[pl.ds((done + k) * rows, size)], osem.at[lax.rem(k, 2)]
        )

    dht_copy = pltpu.make_async_copy(dht_hbm, dht, hsem)
    dh_copy = pltpu.make_async_copy(dh, dh_hbm, hsem)
    part_copy = pltpu.make_async_copy(part_ref, dw_hbm.at[pl.ds(i * rows, rows)], csem)

    @pl.when(i < done)
    def _():
        part_copy.start()

    @pl.when(i == 0)
    def _():
        loss_out[0] = loss_in[0]
        dht_copy.start()

    @pl.when(i == 1)
    def _():
        dht_copy.wait()
        dh[...] = dht[...].T
        dh_copy.start()

    @pl.when(i >= 2)
    def _():
        out_copy(i - 2, rows).wait()

    buf[slot] = jnp.dot(dz_ref[...], h_ref[...], preferred_element_type=jnp.float32)

    @pl.when(i < done)
    def _():
        part_copy.wait()

    @pl.when(i < steps - 1)
    def _():
        out_copy(i, rows).start()

    @pl.when(i == steps - 1)
    def _():
        out_copy(i, final).start()
        out_copy(i - 1, rows).wait()
        out_copy(i, final).wait()
        dh_copy.wait()


def run_weight_grad(rows, done, dz, hidden, part, dht, loss):
    vocab, tok = dz.shape
    d, t = dht.shape
    steps = pl.cdiv(vocab, rows) - done
    assert done <= steps and steps >= 2
    any_spec = pl.BlockSpec(memory_space=pl.ANY)
    smem_spec = pl.BlockSpec(memory_space=pltpu.SMEM)
    return pl.pallas_call(
        functools.partial(weight_grad_kernel, rows, done, vocab),
        grid=(steps,),
        in_specs=[
            pl.BlockSpec((rows, tok), lambda i: (done + i, 0)),
            pl.BlockSpec((tok, d), lambda i: (0, 0), pipeline_mode=pl.Buffered(1)),
            pl.BlockSpec((rows, d), lambda i: (jnp.minimum(i, done - 1), 0)),
            any_spec,
            smem_spec,
        ],
        out_specs=[any_spec, any_spec, smem_spec],
        out_shape=[
            jax.ShapeDtypeStruct((vocab, d), jnp.float32),
            jax.ShapeDtypeStruct((t, d), jnp.float32),
            jax.ShapeDtypeStruct((1,), jnp.float32),
        ],
        scratch_shapes=[
            pltpu.VMEM((2, rows, d), jnp.float32),
            pltpu.VMEM((d, t), jnp.float32),
            pltpu.VMEM((t, d), jnp.float32),
            pltpu.SemaphoreType.DMA((2,)),
            pltpu.SemaphoreType.DMA,
            pltpu.SemaphoreType.DMA,
        ],
        compiler_params=pltpu.CompilerParams(dimension_semantics=("arbitrary",), vmem_limit_bytes=VMEM_LIMIT),
        name="weight_grad",
    )(dz, hidden, part, dht, loss)


def solution(mesh, tile=TILE, rows_w=ROWS):
    n = mesh.shape[AXIS]

    def local_step(hidden, targets, w_blk):
        tgt = targets.reshape(n, 1, hidden.shape[0] // n)
        z, lse, loss = run_stats(n, tile, hidden, tgt, w_blk, 0)
        done = pl.cdiv(w_blk.shape[0], rows_w) // 2
        dht, dz, part = run_hidden_grad(n, tile, rows_w, done, w_blk, z, hidden, lse, tgt, 1)
        dw, dh, loss = run_weight_grad(rows_w, done, dz, hidden, part, dht, loss)
        return loss, dh, dw

    return jax.shard_map(
        local_step,
        mesh=mesh,
        in_specs=(P("data", None), P("data"), P(AXIS, None)),
        out_specs=(P("data"), P(("data", AXIS), None), P(("data", AXIS), None)),
        check_vma=False,
    )
```
